32 devices in a mesh: groups: 2 (over y), seq: 4 (over z), head: 2 (over x), rep: 2 (over core).
Axes of the slice: x: 2, y: 2, z: 4, core: 2. Of those that a mesh axis runs over, the one named last changes fastest.
Arguments:
- queries: bfloat16 [2048, 6144], P(('groups', 'seq', 'rep'), 'head'), parts along dimension 0, may hold values from -150 to 150
- key_tokens: bfloat16 [2048, 6144], P(('groups', 'seq', 'rep'), 'head'), parts along dimension 0, may hold values from -6 to 6
- value_tokens: bfloat16 [2048, 6144], P(('groups', 'seq', 'rep'), 'head'), parts along dimension 0, may hold values from -6 to 6
- stream: bfloat16 [2048, 6144], P(('groups', 'seq', 'rep'), 'head'), parts along dimension 0, may hold values from -6 to 6
- norm_gain: float32 [6144], P('head'), may hold values from 0.1 to 1.9
- latent_weight: bfloat16 [6144, 64], P('head'), may hold values from -0.078125 to 0.078125
- tile_pool: bfloat16 [8, 64, 2, 128], P(('groups', 'seq')), parts along dimension 0, may hold values from -6 to 6
- tile_position: int32 [8], P('groups'), parts along dimension 0, may hold values from 0 to 3, each once
- lift_weight: bfloat16 [64, 512], P(None, ('head', 'rep')), may hold values from -0.75 to 0.75
- lift_bias: float32 [512], P(('head', 'rep')), may hold values from -3 to 3
- conv_weight: bfloat16 [2, 27, 512, 512], P(None, None, ('head', 'rep')), may hold values from -0.0546875 to 0.0546875
Outputs:
- hidden: bfloat16 [2048, 6144], P(('groups', 'seq', 'rep'), 'head'), parts along dimension 0
- latents: float32 [2048, 64], P(('groups', 'seq', 'rep')), parts along dimension 0
- decoded: float32 [1024, 2, 4, 128], P(('groups', 'head', 'rep'), None, 'seq'), parts along dimension 0
The draws below stay inside these ranges and needn't reach their ends.
There are 2 independent parts, one for each index of `groups`. The reference program is written for one: setup_inputs(seed, part) draws one part's arguments, and reference() takes and returns one part's arrays. A program takes and returns all parts, laid end to end along the dimension named above; an argument that names none is the same for every part. Nothing has to cross between parts.
Inputs may be any that keep to these rules, and one draw needn't show every extreme that they name: `tile_position`: each of the 4 grid rows is named by exactly one pool tile.
All inputs are finite; a program needn't handle non-finite values.
Results may differ from the reference program's by a relative error of at most 0.01.
Values may be sent and summed in bfloat16 or wider, within the bound.
No kernel may reach another device: no remote copies, remote signals or barrier semaphores. Data moves between devices by JAX's collectives and lax.ppermute only.
A program may use at most 128 MiB of HBM per device.

```python
import math
import jax
import jax.numpy as jnp
from jax import lax

HEADS = 48
HEAD_DIM = 128
WIDTH = 6144
LATENT = 64
CHANNELS = 512
FRAMES = 2
COLS = 128
DLAYERS = 2
TOKENS = 1024
TILES = 4


def key_draw(key):
    return jnp.clip(jax.random.normal(jax.random.fold_in(key, 102), (TOKENS, WIDTH), jnp.float32), -6.0, 6.0)


def draw_key_tokens(key, part):
    drawn = key_draw(key)
    return drawn.astype(jnp.bfloat16)


def draw_queries(key, part):
    drawn = jnp.clip(2.5 * jax.random.normal(jax.random.fold_in(key, 104), (TOKENS, WIDTH), jnp.float32), -15.0, 15.0)
    return drawn.astype(jnp.bfloat16)


def block_scale(stream_key, extent, pieces, smallest, largest):
    loudness = 1.0
    for axis_at, shards_of in pieces:
        steps = jax.random.uniform(jax.random.fold_in(jax.random.fold_in(stream_key, 6), axis_at), (shards_of,), jnp.float32, smallest / len(pieces), largest / len(pieces))
        loudness = loudness * jnp.repeat(jnp.exp(steps), extent[axis_at] // shards_of).reshape((-1,) + (1,) * (len(extent) - 1 - axis_at))
    return loudness


def noise(own_key, extent, spread, limit, cuts=(), kind=jnp.bfloat16):
    entries = spread * jax.random.normal(own_key, extent, jnp.float32)
    if cuts:
        entries = entries * block_scale(own_key, extent, cuts, -0.22, 0.18)
    return jnp.clip(entries, -limit, limit).astype(kind)


def setup_inputs(seed: int = 0, part: int = 0) -> dict:
    key_of = jax.random.split(jax.random.key(seed), 12)
    own_keys = jax.random.split(jax.random.fold_in(key_of[11], part), 12)
    queries = draw_queries(jax.random.fold_in(jax.random.fold_in(key_of[11], part), 71), part)
    key_tokens = draw_key_tokens(jax.random.fold_in(jax.random.fold_in(key_of[11], part), 71), part)
    value_tokens = noise(own_keys[2], (TOKENS, WIDTH), 1.0, 6.0, ((0, 8), (1, 2)))
    stream = noise(own_keys[3], (TOKENS, WIDTH), 1.0, 6.0, ((0, 8), (1, 2)))
    norm_gain = jnp.clip(1.0 + 0.18 * jax.random.normal(key_of[4], (WIDTH,), jnp.float32), 0.1, 1.9)
    latent_weight = noise(key_of[5], (WIDTH, LATENT), WIDTH ** -0.5, 0.078125, ((0, 2),))
    tile_pool = noise(own_keys[6], (TILES, LATENT, FRAMES, COLS), 1.0, 6.0, ((0, 4),))
    tile_position = jax.random.permutation(own_keys[7], TILES).astype(jnp.int32)
    lift_weight = noise(key_of[8], (LATENT, CHANNELS), LATENT ** -0.5, 0.75, ((1, 4),))
    lift_bias = noise(key_of[9], (CHANNELS,), 0.5, 3.0, ((0, 4),), jnp.float32)
    conv_weight = noise(key_of[10], (DLAYERS, 27, CHANNELS, CHANNELS), (27 * CHANNELS) ** -0.5, 0.0546875, ((2, 4),))
    return {"queries": queries, "key_tokens": key_tokens, "value_tokens": value_tokens, "stream": stream, "norm_gain": norm_gain, "latent_weight": latent_weight, "tile_pool": tile_pool, "tile_position": tile_position, "lift_weight": lift_weight, "lift_bias": lift_bias, "conv_weight": conv_weight}


epsilon = 1e-06

def head_attention(operands):
    query_head, key_head, value_head = operands
    scores = jnp.dot(query_head, key_head.T, preferred_element_type=jnp.float32) * (1.0 / math.sqrt(HEAD_DIM))
    row_peak = lax.optimization_barrier(jnp.max(scores, axis=1, keepdims=True))
    exponent = jnp.exp(scores - row_peak)
    weights = exponent.astype(jnp.bfloat16)
    summed = jnp.dot(weights, value_head, preferred_element_type=jnp.float32)
    return (summed / lax.optimization_barrier(jnp.sum(exponent, axis=1, keepdims=True))).astype(jnp.bfloat16)

def by_heads(matrix):
    return jnp.transpose(matrix.reshape(TOKENS, HEADS, HEAD_DIM), (1, 0, 2))

def reference(queries, key_tokens, value_tokens, stream, norm_gain, latent_weight, tile_pool, tile_position, lift_weight, lift_bias, conv_weight):
    attended = lax.map(head_attention, (by_heads(queries), by_heads(key_tokens), by_heads(value_tokens)))
    attended = jnp.transpose(attended, (1, 0, 2)).reshape(TOKENS, WIDTH)
    hidden = (stream.astype(jnp.float32) + attended.astype(jnp.float32)).astype(jnp.bfloat16)
    widened = hidden.astype(jnp.float32)
    scaled = (widened * norm_gain).astype(jnp.bfloat16)
    projected = jnp.dot(scaled, latent_weight, preferred_element_type=jnp.float32)
    squares = lax.optimization_barrier(jnp.sum(widened * widened, axis=1))
    latents = projected * lax.rsqrt(squares / WIDTH + epsilon)[:, None]
    latent_grid = jnp.zeros((LATENT, FRAMES, TILES, COLS), jnp.bfloat16)
    latent_grid = latent_grid.at[:, :, tile_position.astype(jnp.int32), :].set(jnp.transpose(tile_pool, (1, 2, 0, 3)))
    feature_map = jnp.dot(lift_weight.T, latent_grid.reshape(LATENT, -1), preferred_element_type=jnp.float32) + lift_bias[:, None]
    for layer_index in range(DLAYERS):
        active = jax.nn.silu(feature_map).astype(jnp.bfloat16).reshape(CHANNELS, FRAMES, TILES, COLS)
        padded = jnp.pad(active, ((0, 0), (1, 1), (1, 1), (1, 1)))
        update = jnp.zeros((CHANNELS, FRAMES * TILES * COLS), jnp.float32)
        for frame_off in range(3):
            for row_off in range(3):
                for col_off in range(3):
                    window = padded[:, frame_off:frame_off + FRAMES, row_off:row_off + TILES, col_off:col_off + COLS].reshape(CHANNELS, -1)
                    tap_weight = conv_weight[layer_index, frame_off * 9 + row_off * 3 + col_off]
                    update = update + lax.dot_general(tap_weight, window, (((1,), (0,)), ((), ())), preferred_element_type=jnp.float32)
        feature_map = feature_map + update
    decoded = feature_map.reshape(CHANNELS, FRAMES, TILES, COLS)
    return (hidden, latents, decoded)
```

```python
import math

import jax
import jax.numpy as jnp
from jax import lax
from jax.experimental import pallas as pl
from jax.experimental.pallas import tpu as pltpu
from jax.sharding import PartitionSpec as P

HEAD_DIM = 128
WIDTH = 6144


epsilon = 1e-06
negative = -1e30


def padded(shard, sides, width):
    for axis, dim in sides:
        peers, length = (lax.axis_size(axis), shard.shape[dim])
        up = [(i, (i + 1) % peers) for i in range(peers - 1)]
        down = [(j, i) for i, j in up]
        last = lax.slice_in_dim(shard, length - width, length, axis=dim)
        leading = lax.slice_in_dim(shard, 0, width, axis=dim)
        before = lax.ppermute(last, axis, up)
        after = lax.ppermute(leading, axis, down)
        shard = jnp.concatenate([before, shard, after], axis=dim)
    return shard


def prepare(block_rows):
    row_count = block_rows.shape[0]
    head_count = block_rows.shape[1] // HEAD_DIM
    query_heads = block_rows.reshape(row_count, head_count, HEAD_DIM)
    initial = (
        jnp.full((head_count, row_count), negative, jnp.float32),
        jnp.zeros((head_count, row_count), jnp.float32),
        jnp.zeros((head_count, row_count, HEAD_DIM), jnp.float32),
    )
    return (query_heads, initial)


def make_update(query_heads, state, pieces):
    head_count = query_heads.shape[1]
    factor = 1.0 / math.sqrt(HEAD_DIM)
    running_max, running_sum, accum = state
    key_piece, value_piece = pieces
    piece_rows = key_piece.shape[0]
    key_heads = key_piece.reshape(piece_rows, head_count, HEAD_DIM)
    value_heads = value_piece.reshape(piece_rows, head_count, HEAD_DIM)
    scores = (
        jnp.einsum("qhd,khd->hqk", query_heads, key_heads, preferred_element_type=jnp.float32)
        * factor
    )
    new_max = jnp.maximum(running_max, jnp.max(scores, axis=2))
    exponent = jnp.exp(scores - new_max[:, :, None])
    running_sum = jnp.sum(exponent, axis=2)
    accum = jnp.einsum(
        "hqk,khd->hqd",
        exponent.astype(jnp.bfloat16),
        value_heads,
        preferred_element_type=jnp.float32,
    )
    return (new_max, running_sum, accum)


def finish(state):
    running_max, running_sum, accum = state
    result = accum / running_sum[:, :, None]
    return jnp.transpose(result, (1, 0, 2)).reshape(result.shape[1], -1).astype(jnp.bfloat16)


def shift_columns(window, col_shift):
    if col_shift == 0:
        return window
    edge = jnp.zeros(window.shape[:-1] + (1,), window.dtype)
    if col_shift < 0:
        return jnp.concatenate([edge, window[..., :-1]], axis=-1)
    return jnp.concatenate([window[..., 1:], edge], axis=-1)


def tap_sum(running, piece_block, layer_weight):
    piece_rows = piece_block.shape[0]
    frames = piece_block.shape[1]
    band_rows = piece_block.shape[2] - 2
    framed = jnp.pad(piece_block, ((0, 0), (1, 1), (0, 0), (0, 0)))
    for frame_off in range(3):
        for row_off in range(3):
            for col_off in range(3):
                window = shift_columns(
                    framed[:, frame_off : frame_off + frames, row_off : row_off + band_rows, :],
                    col_off - 1,
                )
                tap_weight = layer_weight[frame_off * 9 + row_off * 3 + col_off]
                running = running + lax.dot_general(
                    tap_weight,
                    window.reshape(piece_rows, -1),
                    (((1,), (0,)), ((), ())),
                    preferred_element_type=jnp.float32,
                )
    return running


def make_pick(tile_position, own_rows, piece_block):
    selector = (own_rows[:, None] == tile_position[None, :]).astype(jnp.bfloat16)
    return jnp.einsum("tp,plfc->lftc", selector, piece_block, preferred_element_type=jnp.float32)


def gathered_shards(
    queries,
    key_tokens,
    value_tokens,
    stream,
    norm_gain,
    latent_weight,
    tile_pool,
    tile_position,
    lift_weight,
    lift_bias,
    conv_weight,
):
    query_heads, initial = prepare(queries)
    state = make_update(
        query_heads,
        initial,
        (
            lax.all_gather(key_tokens, ("seq", "rep"), axis=0, tiled=True),
            lax.all_gather(value_tokens, ("seq", "rep"), axis=0, tiled=True),
        ),
    )
    attended = finish(state)
    combined = stream.astype(jnp.float32) + attended.astype(jnp.float32)
    hidden = combined.astype(jnp.bfloat16)
    widened = hidden.astype(jnp.float32)
    scaled = (widened * norm_gain).astype(jnp.bfloat16)
    partial_proj = jnp.dot(scaled, latent_weight, preferred_element_type=jnp.float32)
    partial_squares = jnp.sum(widened * widened, axis=1)
    projected, squares = (
        lax.psum(partial_proj.astype(jnp.bfloat16), "head").astype(jnp.float32),
        lax.psum(partial_squares.astype(jnp.bfloat16), "head").astype(jnp.float32),
    )
    latents = projected * lax.rsqrt(squares / WIDTH + epsilon)[:, None]
    tiles_here = tile_pool.shape[0]
    frames = tile_pool.shape[2]
    columns = tile_pool.shape[3]
    own_rows = lax.axis_index("seq") * tiles_here + jnp.arange(tiles_here, dtype=jnp.int32)
    collected = make_pick(
        tile_position, own_rows, lax.all_gather(tile_pool, "seq", axis=0, tiled=True)
    )
    latent_grid = collected.astype(jnp.bfloat16)
    channels_here = lift_weight.shape[1]
    feature_map = (
        lax.dot_general(
            lift_weight,
            latent_grid.reshape(latent_grid.shape[0], -1),
            (((0,), (0,)), ((), ())),
            preferred_element_type=jnp.float32,
        )
        + lift_bias[:, None]
    )
    for layer_index in range(conv_weight.shape[0]):
        layer_weight = conv_weight[layer_index]
        active = (
            jax.nn.silu(feature_map)
            .astype(jnp.bfloat16)
            .reshape(channels_here, frames, tiles_here, columns)
        )
        zeros_here = jnp.zeros(feature_map.shape, jnp.float32)
        bordered = padded(active, (("seq", 2),), 1)
        rimmed = lax.all_gather(bordered, ("head", "rep"), axis=0, tiled=True)
        update = tap_sum(zeros_here, rimmed, layer_weight)
        feature_map = feature_map + update
    decoded = feature_map.reshape(channels_here, frames, tiles_here, columns)
    return (hidden, latents, decoded)


def fits(queries, tile_pool, tile_position):
    chips = lax.axis_size("seq")
    heads = queries.shape[1] // HEAD_DIM
    return (
        lax.axis_size("head") == 2
        and lax.axis_size("rep") == 2
        and heads % chips == 0
        and heads // chips >= 2
        and tile_pool.shape[0] == 1
        and tile_pool.shape[2] == 2
        and tile_pool.shape[3] == 128
    )


def whole_vmem(count):
    return [pl.BlockSpec(memory_space=pltpu.VMEM) for _ in range(count)]


def pack(place, sources, tile, shift, chips, per_chip, first, count):
    rows = sources[0].shape[0]
    tile_rows = 0 if tile is None else tile.shape[0]

    def kernel(place_ref, *refs):
        inputs, message, sem = (refs[:-2], refs[-2], refs[-1])
        base = lax.rem(place_ref[0] + shift, chips) * per_chip + first
        copies = []
        for kind in range(3):
            for head in range(count):
                column = pl.multiple_of((base + head) * HEAD_DIM, HEAD_DIM)
                copies.append(
                    pltpu.make_async_copy(
                        inputs[kind].at[:, pl.ds(column, HEAD_DIM)],
                        message.at[pl.ds((kind * count + head) * rows, rows), :],
                        sem.at[len(copies)],
                    )
                )
        if tile is not None:
            copies.append(
                pltpu.make_async_copy(
                    inputs[3],
                    message.at[pl.ds(3 * count * rows, tile_rows), :],
                    sem.at[len(copies)],
                )
            )
        for copy in copies:
            copy.start()
        for copy in copies:
            copy.wait()

    operands = list(sources) + ([] if tile is None else [tile])
    return pl.pallas_call(
        kernel,
        out_shape=jax.ShapeDtypeStruct((3 * count * rows + tile_rows, HEAD_DIM), jnp.bfloat16),
        in_specs=[pl.BlockSpec(memory_space=pltpu.SMEM)]
        + [pl.BlockSpec(memory_space=pl.ANY) for _ in operands],
        out_specs=pl.BlockSpec(memory_space=pl.ANY),
        scratch_shapes=[pltpu.SemaphoreType.DMA((3 * count + 1,))],
        name=f"pack_{first}_{shift}",
    )(place, *operands)


def join(messages, count, rows, tile_rows):
    pieces = len(messages)

    def kernel(*refs):
        inputs, joined = (refs[:-1], refs[-1])
        for head in range(count):
            for kind in range(2):
                for piece in range(pieces):
                    joined[pl.ds(((2 * head + kind) * pieces + piece) * rows, rows), :] = inputs[piece][
                        pl.ds(((kind + 1) * count + head) * rows, rows), :
                    ]
        if tile_rows:
            for piece in range(pieces):
                joined[pl.ds(2 * count * pieces * rows + piece * tile_rows, tile_rows), :] = inputs[piece][
                    pl.ds(3 * count * rows, tile_rows), :
                ]

    return pl.pallas_call(
        kernel,
        out_shape=jax.ShapeDtypeStruct((pieces * (2 * count * rows + tile_rows), HEAD_DIM), jnp.bfloat16),
        in_specs=whole_vmem(pieces),
        out_specs=pl.BlockSpec(memory_space=pltpu.VMEM),
        name=f"join_{count}",
    )(*messages)


def attend(messages, own, partner, count, rows):
    pieces = len(messages)
    factor = math.log2(math.e) / math.sqrt(HEAD_DIM)

    def kernel(*refs):
        inputs, (own_ref, partner_ref), outputs = (refs[:pieces], refs[pieces : pieces + 2], refs[pieces + 2 :])
        length = pieces * rows
        for head in range(count):
            query = jnp.concatenate([m[pl.ds(head * rows, rows), :] for m in inputs], axis=0)
            start = 2 * head * length
            key = jnp.concatenate([own_ref[pl.ds(start, length), :], partner_ref[pl.ds(start, length), :]], axis=0)
            start = start + length
            value = jnp.concatenate([own_ref[pl.ds(start, length), :], partner_ref[pl.ds(start, length), :]], axis=0)
            scores = lax.dot_general(query, key, (((1,), (1,)), ((), ())), preferred_element_type=jnp.float32)
            peak = jnp.max(scores, axis=1, keepdims=True)
            exponent = jnp.exp2((scores - peak) * factor)
            total = jnp.sum(exponent, axis=1, keepdims=True)
            summed = jnp.dot(exponent.astype(jnp.bfloat16), value, preferred_element_type=jnp.float32)
            result = (summed / total).astype(jnp.bfloat16)
            for piece in range(pieces):
                outputs[piece][pl.ds(head * rows, rows), :] = result[piece * rows : (piece + 1) * rows, :]

    shape = jax.ShapeDtypeStruct((count * rows, HEAD_DIM), jnp.bfloat16)
    return pl.pallas_call(
        kernel,
        out_shape=[shape] * pieces,
        in_specs=whole_vmem(pieces + 2),
        out_specs=whole_vmem(pieces),
        name=f"attend_{count}",
    )(*messages, own, partner)


def close(place, chunks, stream, gain, latent_weight, counts, per_chip):
    rows, columns = stream.shape
    latent = latent_weight.shape[1]
    pieces = len(chunks[0])
    flat = [piece for chunk in chunks for piece in chunk]

    def kernel(place_ref, *refs):
        inputs = refs[: len(flat)]
        stream_ref, gain_ref, weight_ref, hidden_ref, part_ref = refs[len(flat) :]
        projected = jnp.zeros((rows, latent), jnp.float32)
        squares = jnp.zeros((rows, HEAD_DIM), jnp.float32)
        for piece in range(pieces):
            base = pl.multiple_of(
                lax.rem(place_ref[0] + piece, pieces) * (per_chip * HEAD_DIM), per_chip * HEAD_DIM
            )
            span = pl.ds(base, per_chip * HEAD_DIM)
            blocks = []
            for index, count in enumerate(counts):
                source = inputs[index * pieces + piece]
                blocks.extend(source[pl.ds(head * rows, rows), :] for head in range(count))
            attended = jnp.concatenate(blocks, axis=1)
            hidden = (stream_ref[:, span].astype(jnp.float32) + attended.astype(jnp.float32)).astype(jnp.bfloat16)
            hidden_ref[:, span] = hidden
            widened = hidden.astype(jnp.float32)
            scaled = (widened * gain_ref[:, span]).astype(jnp.bfloat16)
            projected = projected + jnp.dot(scaled, weight_ref[span, :], preferred_element_type=jnp.float32)
            squared = widened * widened
            for head in range(per_chip):
                squares = squares + squared[:, head * HEAD_DIM : (head + 1) * HEAD_DIM]
        total = jnp.sum(squares, axis=1, keepdims=True)
        part_ref[...] = jnp.concatenate([projected, jnp.broadcast_to(total, (rows, latent))], axis=1)

    return pl.pallas_call(
        kernel,
        out_shape=[
            jax.ShapeDtypeStruct((rows, columns), jnp.bfloat16),
            jax.ShapeDtypeStruct((rows, 2 * latent), jnp.float32),
        ],
        in_specs=[pl.BlockSpec(memory_space=pltpu.SMEM)] + whole_vmem(len(flat) + 3),
        out_specs=whole_vmem(2),
        name="close",
    )(place, *flat, stream, gain, latent_weight)


def silu(value):
    return value / (1.0 + jnp.exp(-value))


def store_shifted(windows, block, active):
    depth, columns = active.shape
    lane = lax.broadcasted_iota(jnp.int32, (depth, columns), 1)
    before = jnp.where(lane == 0, 0.0, pltpu.roll(active, 1, 1))
    after = jnp.where(lane == columns - 1, 0.0, pltpu.roll(active, columns - 1, 1))
    for tap, window in enumerate((before, active, after)):
        windows[pl.ds(tap * depth, depth), pl.ds(block * columns, columns)] = window.astype(jnp.bfloat16)


def frame_taps(weights, windows, frame_tap, width, in_rows, out_rows, totals):
    for row_tap in range(3):
        first = 9 * frame_tap + 3 * row_tap
        taps = jnp.concatenate([weights[first + tap] for tap in range(3)], axis=1)
        for frame in range(2):
            source = frame + frame_tap - 1
            if 0 <= source < 2:
                window = windows[:, pl.ds((source * in_rows + row_tap) * width, out_rows * width)]
                totals[frame] = totals[frame] + jnp.dot(taps, window, preferred_element_type=jnp.float32)
    return totals


def first_layer(place, position, own_tiles, partner_tiles, lift_all, lift_own, conv_weight):
    chips = position.shape[0]
    latent = own_tiles.shape[0] // chips
    width = own_tiles.shape[1]
    channels, own_channels = (lift_all.shape[0], lift_own.shape[0])
    taps = conv_weight.shape[1]

    def kernel(
        place_ref, position_ref, own_ref, partner_ref, all_ref, mine_ref, weight_ref, active_ref, feature_ref,
        weights, windows, sem,
    ):
        third = taps // 3
        copies = [
            pltpu.make_async_copy(
                weight_ref.at[0, pl.ds(part * third, third)], weights.at[pl.ds(part * third, third)], sem.at[part]
            )
            for part in range(3)
        ]
        for copy in copies:
            copy.start()
        row, core = (place_ref[0], place_ref[1])

        def tile_of(source, target):
            picked = jnp.zeros((latent, width), jnp.float32)
            for piece in range(chips):
                tile = source[pl.ds(piece * latent, latent), :].astype(jnp.float32)
                named = position_ref[lax.rem(row + chips - piece, chips)]
                picked = jnp.where(named == target, tile, picked)
            return picked

        weight_all = all_ref[:, :latent].astype(jnp.bfloat16)
        bias_all = all_ref[:, latent : latent + 1]
        grid = [[None] * 5, [None] * 5]
        for offset in range(5):
            target = row + offset - 2
            inside = jnp.logical_and(target >= 0, target < chips)
            mine, other = (tile_of(own_ref, target), tile_of(partner_ref, target))
            grid[0][offset] = jnp.where(core == 0, mine, other).astype(jnp.bfloat16)
            grid[1][offset] = jnp.where(core == 0, other, mine).astype(jnp.bfloat16)
            for frame in range(2):
                lifted = (
                    jnp.dot(weight_all, grid[frame][offset], preferred_element_type=jnp.float32) + bias_all
                )
                active = jnp.where(inside, silu(lifted), 0.0)
                store_shifted(windows, frame * 5 + offset, active)
        weight_own = mine_ref[:, :latent].astype(jnp.bfloat16)
        bias_own = mine_ref[:, latent : latent + 1]
        totals = [jnp.zeros((own_channels, 3 * width), jnp.float32) for _ in range(2)]
        for frame_tap in range(3):
            copies[frame_tap].wait()
            totals = frame_taps(weights, windows, frame_tap, width, 5, 3, totals)
        for frame in range(2):
            near = jnp.concatenate(grid[frame][1:4], axis=1)
            feature = (
                jnp.dot(weight_own, near, preferred_element_type=jnp.float32) + bias_own
            ) + totals[frame]
            feature_ref[:, pl.ds(frame * width, width)] = feature[:, width : 2 * width]
            for offset in range(3):
                target = row + offset - 1
                inside = jnp.logical_and(target >= 0, target < chips)
                block = silu(feature[:, offset * width : (offset + 1) * width])
                active_ref[:, pl.ds((frame * 3 + offset) * width, width)] = jnp.where(
                    inside, block, 0.0
                ).astype(jnp.bfloat16)

    return pl.pallas_call(
        kernel,
        out_shape=[
            jax.ShapeDtypeStruct((own_channels, 6 * width), jnp.bfloat16),
            jax.ShapeDtypeStruct((own_channels, 2 * width), jnp.float32),
        ],
        in_specs=[pl.BlockSpec(memory_space=pltpu.SMEM)] * 2
        + whole_vmem(4)
        + [pl.BlockSpec(memory_space=pl.ANY)],
        out_specs=whole_vmem(2),
        scratch_shapes=[
            pltpu.VMEM((taps, own_channels, channels), jnp.bfloat16),
            pltpu.VMEM((3 * channels, 10 * width), jnp.bfloat16),
            pltpu.SemaphoreType.DMA((3,)),
        ],
        name="first_layer",
    )(place, position, own_tiles, partner_tiles, lift_all, lift_own, conv_weight)


def second_layer(active, feature, conv_weight):
    channels = active.shape[0]
    width = active.shape[1] // 6
    own_channels = feature.shape[0]
    taps = conv_weight.shape[1]

    def kernel(active_ref, feature_ref, weight_ref, decoded_ref, weights, windows, sem):
        third = taps // 3
        copies = [
            pltpu.make_async_copy(
                weight_ref.at[1, pl.ds(part * third, third)], weights.at[pl.ds(part * third, third)], sem.at[part]
            )
            for part in range(3)
        ]
        for copy in copies:
            copy.start()
        for block in range(6):
            store_shifted(windows, block, active_ref[:, pl.ds(block * width, width)].astype(jnp.float32))
        totals = [jnp.zeros((own_channels, width), jnp.float32) for _ in range(2)]
        for frame_tap in range(3):
            copies[frame_tap].wait()
            totals = frame_taps(weights, windows, frame_tap, width, 3, 1, totals)
        for frame in range(2):
            decoded_ref[:, frame, :] = feature_ref[:, pl.ds(frame * width, width)] + totals[frame]

    return pl.pallas_call(
        kernel,
        out_shape=jax.ShapeDtypeStruct((own_channels, 2, width), jnp.float32),
        in_specs=whole_vmem(2) + [pl.BlockSpec(memory_space=pl.ANY)],
        out_specs=pl.BlockSpec(memory_space=pltpu.VMEM),
        scratch_shapes=[
            pltpu.VMEM((taps, own_channels, channels), jnp.bfloat16),
            pltpu.VMEM((3 * channels, 6 * width), jnp.bfloat16),
            pltpu.SemaphoreType.DMA((3,)),
        ],
        name="second_layer",
    )(active, feature, conv_weight)


def exchanged_shards(
    queries,
    key_tokens,
    value_tokens,
    stream,
    norm_gain,
    latent_weight,
    tile_pool,
    tile_position,
    lift_weight,
    lift_bias,
    conv_weight,
):
    chips = lax.axis_size("seq")
    rows = queries.shape[0]
    per_chip = queries.shape[1] // HEAD_DIM // chips
    counts = (per_chip - per_chip // 2, per_chip // 2)
    latent_channels, frames, columns = tile_pool.shape[1:]
    core = lax.axis_index("rep")
    place = jnp.stack([lax.axis_index("seq"), core]).astype(jnp.int32)
    half_tile = jnp.where(core == 0, tile_pool[0, :, 0, :], tile_pool[0, :, 1, :])
    onward = [[(i, (i + shift) % chips) for i in range(chips)] for shift in range(chips)]
    back = [[(j, i) for i, j in pairs] for pairs in onward]
    sources = (queries, key_tokens, value_tokens)
    shifts = (2, 1, 3) if chips == 4 else tuple(range(1, chips))

    def send(first, count, tile):
        arrived = [None] * chips
        for shift in shifts + (0,):
            message = pack(place, sources, tile, shift, chips, per_chip, first, count)
            arrived[shift] = message if shift == 0 else lax.ppermute(message, "seq", onward[shift])
        return arrived

    chunks = [send(0, counts[0], half_tile), send(counts[0], counts[1], None)]

    lift_own = jnp.concatenate(
        [
            lift_weight.T.astype(jnp.float32),
            lift_bias[:, None],
            jnp.zeros((lift_bias.shape[0], 128 - latent_channels - 1), jnp.float32),
        ],
        axis=1,
    )
    lift_all = lax.all_gather(lift_own, ("head", "rep"), axis=0, tiled=True)

    returned = []
    for index, (arrived, count) in enumerate(zip(chunks, counts)):
        tile_rows = latent_channels if index == 0 else 0
        own = join(arrived, count, rows, tile_rows)
        partner = lax.ppermute(own, "rep", [(0, 1), (1, 0)])
        if index == 0:
            own_tiles, partner_tiles = (own[2 * count * chips * rows :], partner[2 * count * chips * rows :])
        results = attend(arrived, own, partner, count, rows)
        home = [None] * chips
        home[0] = results[0]
        for shift in shifts:
            home[shift] = lax.ppermute(results[shift], "seq", back[shift])
        returned.append(home)

    active, feature = first_layer(
        place, tile_position, own_tiles, partner_tiles, lift_all, lift_own, conv_weight
    )
    active_all = lax.all_gather(active, ("head", "rep"), axis=0, tiled=True)
    decoded = second_layer(active_all, feature, conv_weight)[:, :, None, :]

    hidden, part = close(
        place, returned, stream, norm_gain[None, :], latent_weight, counts, per_chip
    )
    part = part + lax.ppermute(part, "head", [(0, 1), (1, 0)])
    latent = latent_weight.shape[1]
    latents = part[:, :latent] * lax.rsqrt(part[:, latent : latent + 1] / WIDTH + epsilon)
    return (hidden, latents, decoded)


def shards(*arrays):
    form = exchanged_shards if fits(arrays[0], arrays[6], arrays[7]) else gathered_shards
    return form(*arrays)


def solution(mesh):
    in_specs = (
        P(("groups", "seq", "rep"), "head"),
        P(("groups", "seq", "rep"), "head"),
        P(("groups", "seq", "rep"), "head"),
        P(("groups", "seq", "rep"), "head"),
        P("head"),
        P("head", None),
        P(("groups", "seq"), None, None, None),
        P("groups"),
        P(None, ("head", "rep")),
        P(("head", "rep")),
        P(None, None, ("head", "rep"), None),
    )
    out_specs = (
        P(("groups", "seq", "rep"), "head"),
        P(("groups", "seq", "rep"), None),
        P(("groups", "head", "rep"), None, "seq", None),
    )
    return jax.shard_map(shards, mesh=mesh, in_specs=in_specs, out_specs=out_specs, check_vma=False)
```

```python
import math

import jax
import jax.numpy as jnp
from jax import lax
from jax.experimental import pallas as pl
from jax.experimental.pallas import tpu as pltpu
from jax.sharding import PartitionSpec as P

HEAD_DIM = 128
WIDTH = 6144


epsilon = 1e-06
negative = -1e30


def padded(shard, sides, width):
    for axis, dim in sides:
        peers, length = (lax.axis_size(axis), shard.shape[dim])
        up = [(i, (i + 1) % peers) for i in range(peers - 1)]
        down = [(j, i) for i, j in up]
        last = lax.slice_in_dim(shard, length - width, length, axis=dim)
        leading = lax.slice_in_dim(shard, 0, width, axis=dim)
        before = lax.ppermute(last, axis, up)
        after = lax.ppermute(leading, axis, down)
        shard = jnp.concatenate([before, shard, after], axis=dim)
    return shard


def prepare(block_rows):
    row_count = block_rows.shape[0]
    head_count = block_rows.shape[1] // HEAD_DIM
    query_heads = block_rows.reshape(row_count, head_count, HEAD_DIM)
    initial = (
        jnp.full((head_count, row_count), negative, jnp.float32),
        jnp.zeros((head_count, row_count), jnp.float32),
        jnp.zeros((head_count, row_count, HEAD_DIM), jnp.float32),
    )
    return (query_heads, initial)


def make_update(query_heads, state, pieces):
    head_count = query_heads.shape[1]
    factor = 1.0 / math.sqrt(HEAD_DIM)
    running_max, running_sum, accum = state
    key_piece, value_piece = pieces
    piece_rows = key_piece.shape[0]
    key_heads = key_piece.reshape(piece_rows, head_count, HEAD_DIM)
    value_heads = value_piece.reshape(piece_rows, head_count, HEAD_DIM)
    scores = (
        jnp.einsum("qhd,khd->hqk", query_heads, key_heads, preferred_element_type=jnp.float32)
        * factor
    )
    new_max = jnp.maximum(running_max, jnp.max(scores, axis=2))
    exponent = jnp.exp(scores - new_max[:, :, None])
    running_sum = jnp.sum(exponent, axis=2)
    accum = jnp.einsum(
        "hqk,khd->hqd",
        exponent.astype(jnp.bfloat16),
        value_heads,
        preferred_element_type=jnp.float32,
    )
    return (new_max, running_sum, accum)


def finish(state):
    _, running_sum, accum = state
    result = accum / running_sum[:, :, None]
    return jnp.transpose(result, (1, 0, 2)).reshape(result.shape[1], -1).astype(jnp.bfloat16)


def shift_columns(window, col_shift):
    if col_shift == 0:
        return window
    edge = jnp.zeros(window.shape[:-1] + (1,), window.dtype)
    if col_shift < 0:
        return jnp.concatenate([edge, window[..., :-1]], axis=-1)
    return jnp.concatenate([window[..., 1:], edge], axis=-1)


def tap_sum(running, piece_block, layer_weight):
    piece_rows = piece_block.shape[0]
    frames = piece_block.shape[1]
    band_rows = piece_block.shape[2] - 2
    framed = jnp.pad(piece_block, ((0, 0), (1, 1), (0, 0), (0, 0)))
    for frame_off in range(3):
        for row_off in range(3):
            for col_off in range(3):
                window = shift_columns(
                    framed[:, frame_off : frame_off + frames, row_off : row_off + band_rows, :],
                    col_off - 1,
                )
                tap_weight = layer_weight[frame_off * 9 + row_off * 3 + col_off]
                running = running + lax.dot_general(
                    tap_weight,
                    window.reshape(piece_rows, -1),
                    (((1,), (0,)), ((), ())),
                    preferred_element_type=jnp.float32,
                )
    return running


def make_pick(tile_position, own_rows, piece_block):
    selector = (own_rows[:, None] == tile_position[None, :]).astype(jnp.bfloat16)
    return jnp.einsum("tp,plfc->lftc", selector, piece_block, preferred_element_type=jnp.float32)


def gathered_shards(
    queries,
    key_tokens,
    value_tokens,
    stream,
    norm_gain,
    latent_weight,
    tile_pool,
    tile_position,
    lift_weight,
    lift_bias,
    conv_weight,
):
    query_heads, initial = prepare(queries)
    state = make_update(
        query_heads,
        initial,
        (
            lax.all_gather(key_tokens, ("seq", "rep"), axis=0, tiled=True),
            lax.all_gather(value_tokens, ("seq", "rep"), axis=0, tiled=True),
        ),
    )
    attended = finish(state)
    combined = stream.astype(jnp.float32) + attended.astype(jnp.float32)
    hidden = combined.astype(jnp.bfloat16)
    widened = hidden.astype(jnp.float32)
    scaled = (widened * norm_gain).astype(jnp.bfloat16)
    partial_proj = jnp.dot(scaled, latent_weight, preferred_element_type=jnp.float32)
    partial_squares = jnp.sum(widened * widened, axis=1)
    projected, squares = (
        lax.psum(partial_proj.astype(jnp.bfloat16), "head").astype(jnp.float32),
        lax.psum(partial_squares.astype(jnp.bfloat16), "head").astype(jnp.float32),
    )
    latents = projected * lax.rsqrt(squares / WIDTH + epsilon)[:, None]
    tiles_here = tile_pool.shape[0]
    frames = tile_pool.shape[2]
    columns = tile_pool.shape[3]
    own_rows = lax.axis_index("seq") * tiles_here + jnp.arange(tiles_here, dtype=jnp.int32)
    collected = make_pick(
        tile_position, own_rows, lax.all_gather(tile_pool, "seq", axis=0, tiled=True)
    )
    latent_grid = collected.astype(jnp.bfloat16)
    channels_here = lift_weight.shape[1]
    feature_map = (
        lax.dot_general(
            lift_weight,
            latent_grid.reshape(latent_grid.shape[0], -1),
            (((0,), (0,)), ((), ())),
            preferred_element_type=jnp.float32,
        )
        + lift_bias[:, None]
    )
    for layer_index in range(conv_weight.shape[0]):
        layer_weight = conv_weight[layer_index]
        active = (
            jax.nn.silu(feature_map)
            .astype(jnp.bfloat16)
            .reshape(channels_here, frames, tiles_here, columns)
        )
        zeros_here = jnp.zeros(feature_map.shape, jnp.float32)
        bordered = padded(active, (("seq", 2),), 1)
        rimmed = lax.all_gather(bordered, ("head", "rep"), axis=0, tiled=True)
        update = tap_sum(zeros_here, rimmed, layer_weight)
        feature_map = feature_map + update
    decoded = feature_map.reshape(channels_here, frames, tiles_here, columns)
    return (hidden, latents, decoded)


def fits(queries, tile_pool):
    chips = lax.axis_size("seq")
    heads = queries.shape[1] // HEAD_DIM
    return (
        lax.axis_size("head") == 2
        and lax.axis_size("rep") == 2
        and heads % chips == 0
        and heads // chips % 2 == 0
        and heads >= chips
        and tile_pool.shape[0] == 1
        and tile_pool.shape[2] == 2
        and tile_pool.shape[3] == 128
    )


def whole_vmem(count):
    return [pl.BlockSpec(memory_space=pltpu.VMEM) for _ in range(count)]


def limit(mebibytes):
    return pltpu.CompilerParams(vmem_limit_bytes=mebibytes * 2**20)


def in_hbm(count):
    return [pl.BlockSpec(memory_space=pltpu.HBM) for _ in range(count)]


def kept(array):
    return pltpu.with_memory_space_constraint(array, pltpu.HBM)


def pack(sources, tile, chips, per_chip, first, count):
    rows = sources[0].shape[0]
    tile_rows = 0 if tile is None else tile.shape[1]
    length = 3 * count * rows + tile_rows

    def kernel(*refs):
        inputs, messages = (refs[: len(operands)], refs[len(operands) : -2])
        blocks, sem = refs[-2:]
        here = lax.axis_index("seq")
        copies = []
        for shift in range(chips):
            chip = lax.rem(here + shift, chips)
            column = pl.multiple_of((chip * per_chip + first) * HEAD_DIM, HEAD_DIM)
            for kind in range(3):
                copies.append(
                    pltpu.make_async_copy(
                        inputs[kind].at[:, pl.ds(column, count * HEAD_DIM)],
                        blocks.at[3 * shift + kind],
                        sem.at[3 * shift + kind],
                    )
                )
        order = [3 * shift + kind for shift in list(range(1, chips)) + [0] for kind in range(3)]
        for at in order:
            copies[at].start()
        if tile is not None:
            core = lax.axis_index("rep")
            frames = [inputs[3][0, :, frame, :].astype(jnp.float32) for frame in range(2)]
            half = jnp.where(core == 0, frames[0], frames[1]).astype(jnp.bfloat16)
            for shift in range(chips):
                messages[shift][pl.ds(3 * count * rows, tile_rows), :] = half
        for at in order:
            shift, kind = divmod(at, 3)
            copies[at].wait()
            for head in range(count):
                messages[shift][pl.ds((kind * count + head) * rows, rows), :] = blocks[
                    at, :, pl.ds(head * HEAD_DIM, HEAD_DIM)
                ]

    operands = [kept(source) for source in sources] + ([] if tile is None else [tile])
    return pl.pallas_call(
        kernel,
        out_shape=[pltpu.VMEM((length, HEAD_DIM), jnp.bfloat16)] * chips,
        in_specs=in_hbm(3) + ([] if tile is None else whole_vmem(1)),
        out_specs=whole_vmem(chips),
        scratch_shapes=[
            pltpu.VMEM((3 * chips, rows, count * HEAD_DIM), jnp.bfloat16),
            pltpu.SemaphoreType.DMA((3 * chips,)),
        ],
        compiler_params=limit(12),
    )(*operands)


def join(messages, count, rows, tile_rows):
    pieces = len(messages)

    def kernel(*refs):
        inputs, joined = (refs[:-1], refs[-1])
        for head in range(count):
            for kind in range(2):
                for piece in range(pieces):
                    joined[pl.ds(((2 * head + kind) * pieces + piece) * rows, rows), :] = inputs[piece][
                        pl.ds(((kind + 1) * count + head) * rows, rows), :
                    ]
        if tile_rows:
            for piece in range(pieces):
                joined[pl.ds(2 * count * pieces * rows + piece * tile_rows, tile_rows), :] = inputs[piece][
                    pl.ds(3 * count * rows, tile_rows), :
                ]

    return pl.pallas_call(
        kernel,
        out_shape=jax.ShapeDtypeStruct((pieces * (2 * count * rows + tile_rows), HEAD_DIM), jnp.bfloat16),
        in_specs=whole_vmem(pieces),
        out_specs=pl.BlockSpec(memory_space=pltpu.VMEM),
        compiler_params=limit(8),
    )(*messages)


def attend(messages, own, partner, count, rows):
    pieces = len(messages)
    factor = math.log2(math.e) / math.sqrt(HEAD_DIM)

    def kernel(*refs):
        inputs, (own_ref, partner_ref), outputs = (refs[:pieces], refs[pieces : pieces + 2], refs[pieces + 2 :])
        length = pieces * rows
        for head in range(count):
            query = jnp.concatenate([m[pl.ds(head * rows, rows), :] for m in inputs], axis=0)
            start = 2 * head * length
            key = jnp.concatenate([own_ref[pl.ds(start, length), :], partner_ref[pl.ds(start, length), :]], axis=0)
            start = start + length
            value = jnp.concatenate([own_ref[pl.ds(start, length), :], partner_ref[pl.ds(start, length), :]], axis=0)
            scores = lax.dot_general(query, key, (((1,), (1,)), ((), ())), preferred_element_type=jnp.float32)
            peak = jnp.max(scores, axis=1, keepdims=True)
            exponent = jnp.exp2((scores - peak) * factor)
            total = jnp.sum(exponent, axis=1, keepdims=True)
            summed = jnp.dot(exponent.astype(jnp.bfloat16), value, preferred_element_type=jnp.float32)
            result = (summed / total).astype(jnp.bfloat16)
            for piece in range(pieces):
                outputs[piece][pl.ds(head * rows, rows), :] = result[piece * rows : (piece + 1) * rows, :]

    shape = jax.ShapeDtypeStruct((count * rows, HEAD_DIM), jnp.bfloat16)
    return pl.pallas_call(
        kernel,
        out_shape=[shape] * pieces,
        in_specs=whole_vmem(pieces + 2),
        out_specs=whole_vmem(pieces),
        compiler_params=limit(24),
    )(*messages, own, partner)


def close(chunks, stream, gain, latent_weight, counts, per_chip):
    rows, columns = stream.shape
    latent = latent_weight.shape[0]
    pieces = len(chunks[0])
    flat = [piece for chunk in chunks for piece in chunk]

    def kernel(*refs):
        here = lax.axis_index("seq")
        inputs = refs[: len(flat)]
        stream_ref, gain_ref, weight_ref, hidden_ref, part_ref = refs[len(flat) :]
        projected = jnp.zeros((latent, rows), jnp.float32)
        squares = jnp.zeros((rows, HEAD_DIM), jnp.float32)
        for piece in range(pieces):
            base = pl.multiple_of(
                lax.rem(here + piece, pieces) * (per_chip * HEAD_DIM), per_chip * HEAD_DIM
            )
            span = pl.ds(base, per_chip * HEAD_DIM)
            blocks = []
            for index, count in enumerate(counts):
                source = inputs[index * pieces + piece]
                blocks.extend(source[pl.ds(head * rows, rows), :] for head in range(count))
            attended = jnp.concatenate(blocks, axis=1)
            hidden = (stream_ref[:, span].astype(jnp.float32) + attended.astype(jnp.float32)).astype(jnp.bfloat16)
            hidden_ref[:, span] = hidden
            widened = hidden.astype(jnp.float32)
            scaled = (widened * gain_ref[:, span]).astype(jnp.bfloat16)
            projected = projected + lax.dot_general(
                weight_ref[:, span], scaled, (((1,), (1,)), ((), ())), preferred_element_type=jnp.float32
            )
            squared = widened * widened
            for head in range(per_chip):
                squares = squares + squared[:, head * HEAD_DIM : (head + 1) * HEAD_DIM]
        total = jnp.sum(squares.T, axis=0, keepdims=True)
        part_ref[pl.ds(0, latent), :] = projected
        part_ref[pl.ds(latent, 8), :] = jnp.broadcast_to(total, (8, rows))

    return pl.pallas_call(
        kernel,
        out_shape=[
            jax.ShapeDtypeStruct((rows, columns), jnp.bfloat16),
            jax.ShapeDtypeStruct((latent + 8, rows), jnp.float32),
        ],
        in_specs=whole_vmem(len(flat) + 3),
        out_specs=whole_vmem(2),
        compiler_params=limit(12),
        name="close",
    )(*flat, stream, gain, latent_weight)


def silu(value):
    return value / (1.0 + jnp.exp(-value))


def store_shifted(windows, block, active):
    depth, columns = active.shape
    lane = lax.broadcasted_iota(jnp.int32, (depth, columns), 1)
    before = jnp.where(lane == 0, 0.0, pltpu.roll(active, 1, 1))
    after = jnp.where(lane == columns - 1, 0.0, pltpu.roll(active, columns - 1, 1))
    for tap, window in enumerate((before, active, after)):
        windows[pl.ds(tap * depth, depth), pl.ds(block * columns, columns)] = window.astype(jnp.bfloat16)


def frame_taps(weights, windows, frame_tap, width, in_rows, out_rows, totals):
    for row_tap in range(3):
        first = 9 * frame_tap + 3 * row_tap
        taps = jnp.concatenate([weights[first + tap] for tap in range(3)], axis=1)
        for frame in range(2):
            source = frame + frame_tap - 1
            if 0 <= source < 2:
                window = windows[:, pl.ds((source * in_rows + row_tap) * width, out_rows * width)]
                totals[frame] = totals[frame] + jnp.dot(taps, window, preferred_element_type=jnp.float32)
    return totals


def first_layer(position, own_tiles, partner_tiles, lift_all, lift_own, conv_weight):
    chips = position.shape[0]
    latent = own_tiles.shape[0] // chips
    width = own_tiles.shape[1]
    channels, own_channels = (lift_all.shape[0], lift_own.shape[0])
    taps = conv_weight.shape[1]

    def kernel(
        position_ref, own_ref, partner_ref, all_ref, mine_ref, weight_ref, active_ref, feature_ref,
        weights, windows, sem,
    ):
        third = taps // 3
        copies = [
            pltpu.make_async_copy(
                weight_ref.at[0, pl.ds(part * third, third)], weights.at[pl.ds(part * third, third)], sem.at[part]
            )
            for part in range(3)
        ]
        for copy in copies:
            copy.start()
        row, core = (lax.axis_index("seq"), lax.axis_index("rep"))

        def tile_of(source, target):
            picked = jnp.zeros((latent, width), jnp.float32)
            for piece in range(chips):
                tile = source[pl.ds(piece * latent, latent), :].astype(jnp.float32)
                named = position_ref[lax.rem(row + chips - piece, chips)]
                picked = jnp.where(named == target, tile, picked)
            return picked

        weight_all = all_ref[:, :latent].astype(jnp.bfloat16)
        bias_all = all_ref[:, latent : latent + 1]
        grid = [[None] * 5, [None] * 5]
        for offset in range(5):
            target = row + offset - 2
            inside = jnp.logical_and(target >= 0, target < chips)
            mine, other = (tile_of(own_ref, target), tile_of(partner_ref, target))
            grid[0][offset] = jnp.where(core == 0, mine, other).astype(jnp.bfloat16)
            grid[1][offset] = jnp.where(core == 0, other, mine).astype(jnp.bfloat16)
            for frame in range(2):
                lifted = (
                    jnp.dot(weight_all, grid[frame][offset], preferred_element_type=jnp.float32) + bias_all
                )
                active = jnp.where(inside, silu(lifted), 0.0)
                store_shifted(windows, frame * 5 + offset, active)
        weight_own = mine_ref[:, :latent].astype(jnp.bfloat16)
        bias_own = mine_ref[:, latent : latent + 1]
        totals = [jnp.zeros((own_channels, 3 * width), jnp.float32) for _ in range(2)]
        for frame_tap in range(3):
            copies[frame_tap].wait()
            totals = frame_taps(weights, windows, frame_tap, width, 5, 3, totals)
        for frame in range(2):
            near = jnp.concatenate(grid[frame][1:4], axis=1)
            feature = (
                jnp.dot(weight_own, near, preferred_element_type=jnp.float32) + bias_own
            ) + totals[frame]
            feature_ref[:, pl.ds(frame * width, width)] = feature[:, width : 2 * width]
            for offset in range(3):
                target = row + offset - 1
                inside = jnp.logical_and(target >= 0, target < chips)
                block = silu(feature[:, offset * width : (offset + 1) * width])
                active_ref[:, pl.ds((frame * 3 + offset) * width, width)] = jnp.where(
                    inside, block, 0.0
                ).astype(jnp.bfloat16)

    return pl.pallas_call(
        kernel,
        out_shape=[
            jax.ShapeDtypeStruct((own_channels, 6 * width), jnp.bfloat16),
            jax.ShapeDtypeStruct((own_channels, 2 * width), jnp.float32),
        ],
        in_specs=[pl.BlockSpec(memory_space=pltpu.SMEM)] + whole_vmem(4) + in_hbm(1),
        out_specs=whole_vmem(2),
        scratch_shapes=[
            pltpu.VMEM((taps, own_channels, channels), jnp.bfloat16),
            pltpu.VMEM((3 * channels, 10 * width), jnp.bfloat16),
            pltpu.SemaphoreType.DMA((3,)),
        ],
        compiler_params=limit(24),
        name="first_layer",
    )(position, own_tiles, partner_tiles, lift_all, lift_own, kept(conv_weight))


def second_layer(active, feature, conv_weight):
    channels = active.shape[0]
    width = active.shape[1] // 6
    own_channels = feature.shape[0]
    taps = conv_weight.shape[1]

    def kernel(active_ref, feature_ref, weight_ref, decoded_ref, weights, windows, sem):
        third = taps // 3
        copies = [
            pltpu.make_async_copy(
                weight_ref.at[1, pl.ds(part * third, third)], weights.at[pl.ds(part * third, third)], sem.at[part]
            )
            for part in range(3)
        ]
        for copy in copies:
            copy.start()
        for block in range(6):
            store_shifted(windows, block, active_ref[:, pl.ds(block * width, width)].astype(jnp.float32))
        totals = [jnp.zeros((own_channels, width), jnp.float32) for _ in range(2)]
        for frame_tap in range(3):
            copies[frame_tap].wait()
            totals = frame_taps(weights, windows, frame_tap, width, 3, 1, totals)
        for frame in range(2):
            decoded_ref[:, frame, :] = feature_ref[:, pl.ds(frame * width, width)] + totals[frame]

    return pl.pallas_call(
        kernel,
        out_shape=jax.ShapeDtypeStruct((own_channels, 2, width), jnp.float32),
        in_specs=whole_vmem(2) + in_hbm(1),
        out_specs=pl.BlockSpec(memory_space=pltpu.VMEM),
        scratch_shapes=[
            pltpu.VMEM((taps, own_channels, channels), jnp.bfloat16),
            pltpu.VMEM((3 * channels, 6 * width), jnp.bfloat16),
            pltpu.SemaphoreType.DMA((3,)),
        ],
        compiler_params=limit(16),
        name="second_layer",
    )(active, feature, kept(conv_weight))


def exchanged_shards(
    queries,
    key_tokens,
    value_tokens,
    stream,
    norm_gain,
    latent_weight,
    tile_pool,
    tile_position,
    lift_weight,
    lift_bias,
    conv_weight,
):
    chips = lax.axis_size("seq")
    rows = queries.shape[0]
    per_chip = queries.shape[1] // HEAD_DIM // chips
    count = per_chip // 2
    latent_channels = tile_pool.shape[1]
    onward = [[(i, (i + shift) % chips) for i in range(chips)] for shift in range(chips)]
    back = [[(j, i) for i, j in pairs] for pairs in onward]
    swap = [(0, 1), (1, 0)]
    sources = (queries, key_tokens, value_tokens)

    def send(messages):
        arrived = [messages[0]]
        for shift in range(1, chips):
            arrived.append(lax.ppermute(messages[shift], "seq", onward[shift]))
        return arrived

    def give_back(results):
        home = [results[0]]
        for shift in range(1, chips):
            home.append(lax.ppermute(results[shift], "seq", back[shift]))
        return home

    early = pack(sources, tile_pool, chips, per_chip, 0, count)
    late = pack(sources, None, chips, per_chip, count, count)
    early_in, late_in = (send(early), send(late))

    lift_weight, lift_bias, _ = lax.optimization_barrier((lift_weight, lift_bias, late[0]))
    lift_own = jnp.concatenate(
        [
            lift_weight.T.astype(jnp.float32),
            lift_bias[:, None],
            jnp.zeros((lift_bias.shape[0], 128 - latent_channels - 1), jnp.float32),
        ],
        axis=1,
    )
    lift_all = lax.all_gather(lift_own, ("head", "rep"), axis=0, tiled=True)

    early_in, lift_all = lax.optimization_barrier((early_in, lift_all))
    own = join(early_in, count, rows, latent_channels)
    partner = lax.ppermute(own, "rep", swap)
    tiles_at = 2 * count * chips * rows
    early_out = attend(early_in, own, partner, count, rows)
    early_home = give_back(early_out)

    own, partner, _ = lax.optimization_barrier((own, partner, early_out[0]))
    active, feature = first_layer(tile_position, own[tiles_at:], partner[tiles_at:], lift_all, lift_own, conv_weight)
    active_all = lax.all_gather(active, ("head", "rep"), axis=0, tiled=True)

    late_in, active_all = lax.optimization_barrier((late_in, active_all))
    own = join(late_in, count, rows, 0)
    partner = lax.ppermute(own, "rep", swap)
    late_out = attend(late_in, own, partner, count, rows)
    late_home = give_back(late_out)

    active_all, _ = lax.optimization_barrier((active_all, late_out[0]))
    decoded = second_layer(active_all, feature, conv_weight)
    decoded = decoded[:, :, None, :]

    hidden, part = close(
        (early_home, late_home), stream, norm_gain[None, :], latent_weight.T, (count, count), per_chip
    )
    part = part + lax.ppermute(part, "head", swap)
    latent = latent_weight.shape[1]
    latents = part[:latent] * lax.rsqrt(part[latent : latent + 1] / WIDTH + epsilon)
    return (hidden, latents.T, decoded)


def shards(*arrays):
    form = exchanged_shards if fits(arrays[0], arrays[6]) else gathered_shards
    return form(*arrays)


def solution(mesh):
    in_specs = (
        P(("groups", "seq", "rep"), "head"),
        P(("groups", "seq", "rep"), "head"),
        P(("groups", "seq", "rep"), "head"),
        P(("groups", "seq", "rep"), "head"),
        P("head"),
        P("head", None),
        P(("groups", "seq"), None, None, None),
        P("groups"),
        P(None, ("head", "rep")),
        P(("head", "rep")),
        P(None, None, ("head", "rep"), None),
    )
    out_specs = (
        P(("groups", "seq", "rep"), "head"),
        P(("groups", "seq", "rep"), None),
        P(("groups", "head", "rep"), None, "seq", None),
    )
    return jax.shard_map(shards, mesh=mesh, in_specs=in_specs, out_specs=out_specs, check_vma=False)
```

```python
import math

import jax
import jax.numpy as jnp
from jax import lax
from jax.experimental import pallas as pl
from jax.experimental.pallas import tpu as pltpu
from jax.sharding import PartitionSpec as P

HEAD_DIM = 128
WIDTH = 6144


epsilon = 1e-06
negative = -1e30


def padded(shard, sides, width):
    for axis, dim in sides:
        peers, length = (lax.axis_size(axis), shard.shape[dim])
        up = [(i, (i + 1) % peers) for i in range(peers - 1)]
        down = [(j, i) for i, j in up]
        last = lax.slice_in_dim(shard, length - width, length, axis=dim)
        leading = lax.slice_in_dim(shard, 0, width, axis=dim)
        before = lax.ppermute(last, axis, up)
        after = lax.ppermute(leading, axis, down)
        shard = jnp.concatenate([before, shard, after], axis=dim)
    return shard


def prepare(block_rows):
    row_count = block_rows.shape[0]
    head_count = block_rows.shape[1] // HEAD_DIM
    query_heads = block_rows.reshape(row_count, head_count, HEAD_DIM)
    initial = (
        jnp.full((head_count, row_count), negative, jnp.float32),
        jnp.zeros((head_count, row_count), jnp.float32),
        jnp.zeros((head_count, row_count, HEAD_DIM), jnp.float32),
    )
    return (query_heads, initial)


def make_update(query_heads, state, pieces):
    head_count = query_heads.shape[1]
    factor = 1.0 / math.sqrt(HEAD_DIM)
    running_max, running_sum, accum = state
    key_piece, value_piece = pieces
    piece_rows = key_piece.shape[0]
    key_heads = key_piece.reshape(piece_rows, head_count, HEAD_DIM)
    value_heads = value_piece.reshape(piece_rows, head_count, HEAD_DIM)
    scores = (
        jnp.einsum("qhd,khd->hqk", query_heads, key_heads, preferred_element_type=jnp.float32)
        * factor
    )
    new_max = jnp.maximum(running_max, jnp.max(scores, axis=2))
    exponent = jnp.exp(scores - new_max[:, :, None])
    running_sum = jnp.sum(exponent, axis=2)
    accum = jnp.einsum(
        "hqk,khd->hqd",
        exponent.astype(jnp.bfloat16),
        value_heads,
        preferred_element_type=jnp.float32,
    )
    return (new_max, running_sum, accum)


def finish(state):
    _, running_sum, accum = state
    result = accum / running_sum[:, :, None]
    return jnp.transpose(result, (1, 0, 2)).reshape(result.shape[1], -1).astype(jnp.bfloat16)


def shift_columns(window, col_shift):
    if col_shift == 0:
        return window
    edge = jnp.zeros(window.shape[:-1] + (1,), window.dtype)
    if col_shift < 0:
        return jnp.concatenate([edge, window[..., :-1]], axis=-1)
    return jnp.concatenate([window[..., 1:], edge], axis=-1)


def tap_sum(running, piece_block, layer_weight):
    piece_rows = piece_block.shape[0]
    frames = piece_block.shape[1]
    band_rows = piece_block.shape[2] - 2
    framed = jnp.pad(piece_block, ((0, 0), (1, 1), (0, 0), (0, 0)))
    for frame_off in range(3):
        for row_off in range(3):
            for col_off in range(3):
                window = shift_columns(
                    framed[:, frame_off : frame_off + frames, row_off : row_off + band_rows, :],
                    col_off - 1,
                )
                tap_weight = layer_weight[frame_off * 9 + row_off * 3 + col_off]
                running = running + lax.dot_general(
                    tap_weight,
                    window.reshape(piece_rows, -1),
                    (((1,), (0,)), ((), ())),
                    preferred_element_type=jnp.float32,
                )
    return running


def make_pick(tile_position, own_rows, piece_block):
    selector = (own_rows[:, None] == tile_position[None, :]).astype(jnp.bfloat16)
    return jnp.einsum("tp,plfc->lftc", selector, piece_block, preferred_element_type=jnp.float32)


def gathered_shards(
    queries,
    key_tokens,
    value_tokens,
    stream,
    norm_gain,
    latent_weight,
    tile_pool,
    tile_position,
    lift_weight,
    lift_bias,
    conv_weight,
):
    query_heads, initial = prepare(queries)
    state = make_update(
        query_heads,
        initial,
        (
            lax.all_gather(key_tokens, ("seq", "rep"), axis=0, tiled=True),
            lax.all_gather(value_tokens, ("seq", "rep"), axis=0, tiled=True),
        ),
    )
    attended = finish(state)
    combined = stream.astype(jnp.float32) + attended.astype(jnp.float32)
    hidden = combined.astype(jnp.bfloat16)
    widened = hidden.astype(jnp.float32)
    scaled = (widened * norm_gain).astype(jnp.bfloat16)
    partial_proj = jnp.dot(scaled, latent_weight, preferred_element_type=jnp.float32)
    partial_squares = jnp.sum(widened * widened, axis=1)
    projected, squares = (
        lax.psum(partial_proj.astype(jnp.bfloat16), "head").astype(jnp.float32),
        lax.psum(partial_squares.astype(jnp.bfloat16), "head").astype(jnp.float32),
    )
    latents = projected * lax.rsqrt(squares / WIDTH + epsilon)[:, None]
    tiles_here = tile_pool.shape[0]
    frames = tile_pool.shape[2]
    columns = tile_pool.shape[3]
    own_rows = lax.axis_index("seq") * tiles_here + jnp.arange(tiles_here, dtype=jnp.int32)
    collected = make_pick(
        tile_position, own_rows, lax.all_gather(tile_pool, "seq", axis=0, tiled=True)
    )
    latent_grid = collected.astype(jnp.bfloat16)
    channels_here = lift_weight.shape[1]
    feature_map = (
        lax.dot_general(
            lift_weight,
            latent_grid.reshape(latent_grid.shape[0], -1),
            (((0,), (0,)), ((), ())),
            preferred_element_type=jnp.float32,
        )
        + lift_bias[:, None]
    )
    for layer_index in range(conv_weight.shape[0]):
        layer_weight = conv_weight[layer_index]
        active = (
            jax.nn.silu(feature_map)
            .astype(jnp.bfloat16)
            .reshape(channels_here, frames, tiles_here, columns)
        )
        zeros_here = jnp.zeros(feature_map.shape, jnp.float32)
        bordered = padded(active, (("seq", 2),), 1)
        rimmed = lax.all_gather(bordered, ("head", "rep"), axis=0, tiled=True)
        update = tap_sum(zeros_here, rimmed, layer_weight)
        feature_map = feature_map + update
    decoded = feature_map.reshape(channels_here, frames, tiles_here, columns)
    return (hidden, latents, decoded)


def fits(queries, tile_pool):
    chips = lax.axis_size("seq")
    heads = queries.shape[1] // HEAD_DIM
    return (
        lax.axis_size("head") == 2
        and lax.axis_size("rep") == 2
        and heads % chips == 0
        and heads // chips % 2 == 0
        and heads >= chips
        and tile_pool.shape[0] == 1
        and tile_pool.shape[2] == 2
        and tile_pool.shape[3] == 128
    )


def ring_of(chips):
    return (0, 2, 3, 1) if chips == 4 else tuple(range(chips))


def neighbour(chips, here, shift):
    ring = ring_of(chips)
    target = jnp.int32(0)
    for at, chip in enumerate(ring):
        target = jnp.where(here == chip, jnp.int32(ring[(at + shift) % chips]), target)
    return target


def whole_vmem(count):
    return [pl.BlockSpec(memory_space=pltpu.VMEM) for _ in range(count)]


def limit(mebibytes):
    return pltpu.CompilerParams(vmem_limit_bytes=mebibytes * 2**20)


def in_hbm(count):
    return [pl.BlockSpec(memory_space=pltpu.HBM) for _ in range(count)]


def kept(array):
    return pltpu.with_memory_space_constraint(array, pltpu.HBM)


def pack(sources, tile, chips, per_chip, first, count):
    rows = sources[0].shape[0]
    tile_rows = 0 if tile is None else tile.shape[1]
    length = 3 * count * rows + tile_rows

    def kernel(*refs):
        inputs, messages = (refs[: len(operands)], refs[len(operands) : len(operands) + chips])
        blocks, sem, *extra = refs[len(operands) + chips :]
        here = lax.axis_index("seq")
        copies = []
        for shift in range(chips):
            chip = neighbour(chips, here, shift)
            column = pl.multiple_of((chip * per_chip + first) * HEAD_DIM, HEAD_DIM)
            for kind in range(3):
                copies.append(
                    pltpu.make_async_copy(
                        inputs[kind].at[:, pl.ds(column, count * HEAD_DIM)],
                        blocks.at[3 * shift + kind],
                        sem.at[3 * shift + kind],
                    )
                )
        order = [3 * shift + kind for shift in list(range(1, chips)) + [0] for kind in range(3)]
        if tile is not None:
            tile_block, tile_sem = extra
            tile_copy = pltpu.make_async_copy(inputs[3], tile_block, tile_sem)
            tile_copy.start()
        for at in order:
            copies[at].start()
        if tile is not None:
            core = lax.axis_index("rep")
            tile_copy.wait()
            frames = [tile_block[0, :, frame, :].astype(jnp.float32) for frame in range(2)]
            half = jnp.where(core == 0, frames[0], frames[1]).astype(jnp.bfloat16)
            for shift in range(chips):
                messages[shift][pl.ds(3 * count * rows, tile_rows), :] = half
        for at in order:
            shift, kind = divmod(at, 3)
            copies[at].wait()
            for head in range(count):
                messages[shift][pl.ds((kind * count + head) * rows, rows), :] = blocks[
                    at, :, pl.ds(head * HEAD_DIM, HEAD_DIM)
                ]

    operands = [kept(source) for source in sources] + ([] if tile is None else [kept(tile)])
    extra_scratch = [] if tile is None else [pltpu.VMEM(tile.shape, tile.dtype), pltpu.SemaphoreType.DMA]
    return pl.pallas_call(
        kernel,
        out_shape=[pltpu.VMEM((length, HEAD_DIM), jnp.bfloat16)] * chips,
        in_specs=in_hbm(len(operands)),
        out_specs=whole_vmem(chips),
        scratch_shapes=[
            pltpu.VMEM((3 * chips, rows, count * HEAD_DIM), jnp.bfloat16),
            pltpu.SemaphoreType.DMA((3 * chips,)),
        ]
        + extra_scratch,
        compiler_params=limit(12),
    )(*operands)


def join(messages, count, rows, tile_rows):
    pieces = len(messages)

    def kernel(*refs):
        inputs, joined = (refs[:-1], refs[-1])
        for head in range(count):
            for kind in range(2):
                for piece in range(pieces):
                    joined[pl.ds(((2 * head + kind) * pieces + piece) * rows, rows), :] = inputs[piece][
                        pl.ds(((kind + 1) * count + head) * rows, rows), :
                    ]
        if tile_rows:
            for piece in range(pieces):
                joined[pl.ds(2 * count * pieces * rows + piece * tile_rows, tile_rows), :] = inputs[piece][
                    pl.ds(3 * count * rows, tile_rows), :
                ]

    return pl.pallas_call(
        kernel,
        out_shape=jax.ShapeDtypeStruct((pieces * (2 * count * rows + tile_rows), HEAD_DIM), jnp.bfloat16),
        in_specs=whole_vmem(pieces),
        out_specs=pl.BlockSpec(memory_space=pltpu.VMEM),
        compiler_params=limit(8),
    )(*messages)


def attend(messages, own, partner, count, rows):
    pieces = len(messages)
    factor = math.log2(math.e) / math.sqrt(HEAD_DIM)

    def kernel(*refs):
        inputs, (own_ref, partner_ref), outputs = (refs[:pieces], refs[pieces : pieces + 2], refs[pieces + 2 :])
        length = pieces * rows
        for head in range(count):
            query = jnp.concatenate([m[pl.ds(head * rows, rows), :] for m in inputs], axis=0)
            start = 2 * head * length
            key = jnp.concatenate([own_ref[pl.ds(start, length), :], partner_ref[pl.ds(start, length), :]], axis=0)
            start = start + length
            value = jnp.concatenate([own_ref[pl.ds(start, length), :], partner_ref[pl.ds(start, length), :]], axis=0)
            scores = lax.dot_general(query, key, (((1,), (1,)), ((), ())), preferred_element_type=jnp.float32)
            peak = jnp.max(scores, axis=1, keepdims=True)
            exponent = jnp.exp2((scores - peak) * factor)
            total = jnp.sum(exponent, axis=1, keepdims=True)
            summed = jnp.dot(exponent.astype(jnp.bfloat16), value, preferred_element_type=jnp.float32)
            result = (summed / total).astype(jnp.bfloat16)
            for piece in range(pieces):
                outputs[piece][pl.ds(head * rows, rows), :] = result[piece * rows : (piece + 1) * rows, :]

    shape = jax.ShapeDtypeStruct((count * rows, HEAD_DIM), jnp.bfloat16)
    return pl.pallas_call(
        kernel,
        out_shape=[shape] * pieces,
        in_specs=whole_vmem(pieces + 2),
        out_specs=whole_vmem(pieces),
        compiler_params=limit(24),
    )(*messages, own, partner)


def close(chunks, stream, gain, latent_weight, counts, per_chip):
    rows, columns = stream.shape
    latent = latent_weight.shape[0]
    pieces = len(chunks[0])
    flat = [piece for chunk in chunks for piece in chunk]

    def kernel(*refs):
        here = lax.axis_index("seq")
        inputs = refs[: len(flat)]
        stream_ref, gain_ref, weight_ref, hidden_ref, part_ref = refs[len(flat) :]
        projected = jnp.zeros((latent, rows), jnp.float32)
        squares = jnp.zeros((rows, HEAD_DIM), jnp.float32)
        for piece in range(pieces):
            base = pl.multiple_of(
                neighbour(pieces, here, piece) * (per_chip * HEAD_DIM), per_chip * HEAD_DIM
            )
            span = pl.ds(base, per_chip * HEAD_DIM)
            blocks = []
            for index, count in enumerate(counts):
                source = inputs[index * pieces + piece]
                blocks.extend(source[pl.ds(head * rows, rows), :] for head in range(count))
            attended = jnp.concatenate(blocks, axis=1)
            hidden = (stream_ref[:, span].astype(jnp.float32) + attended.astype(jnp.float32)).astype(jnp.bfloat16)
            hidden_ref[:, span] = hidden
            widened = hidden.astype(jnp.float32)
            scaled = (widened * gain_ref[:, span]).astype(jnp.bfloat16)
            projected = projected + lax.dot_general(
                weight_ref[:, span], scaled, (((1,), (1,)), ((), ())), preferred_element_type=jnp.float32
            )
            squared = widened * widened
            for head in range(per_chip):
                squares = squares + squared[:, head * HEAD_DIM : (head + 1) * HEAD_DIM]
        total = jnp.sum(squares.T, axis=0, keepdims=True)
        part_ref[pl.ds(0, latent), :] = projected
        part_ref[pl.ds(latent, 8), :] = jnp.broadcast_to(total, (8, rows))

    return pl.pallas_call(
        kernel,
        out_shape=[
            jax.ShapeDtypeStruct((rows, columns), jnp.bfloat16),
            jax.ShapeDtypeStruct((latent + 8, rows), jnp.float32),
        ],
        in_specs=whole_vmem(len(flat) + 3),
        out_specs=whole_vmem(2),
        compiler_params=limit(12),
        name="close",
    )(*flat, stream, gain, latent_weight)


def silu(value):
    return value / (1.0 + jnp.exp(-value))


def store_shifted(windows, block, active, first, channels):
    depth, columns = active.shape
    lane = lax.broadcasted_iota(jnp.int32, (depth, columns), 1)
    before = jnp.where(lane == 0, 0.0, pltpu.roll(active, 1, 1))
    after = jnp.where(lane == columns - 1, 0.0, pltpu.roll(active, columns - 1, 1))
    for tap, window in enumerate((before, active, after)):
        at = pl.ds(tap * channels + first, depth)
        windows[at, pl.ds(block * columns, columns)] = window.astype(jnp.bfloat16)


def frame_taps(weights, windows, frame_tap, width, in_rows, out_rows, totals):
    for row_tap in range(3):
        first = 9 * frame_tap + 3 * row_tap
        taps = jnp.concatenate([weights[first + tap] for tap in range(3)], axis=1)
        for frame in range(2):
            source = frame + frame_tap - 1
            if 0 <= source < 2:
                window = windows[:, pl.ds((source * in_rows + row_tap) * width, out_rows * width)]
                totals[frame] = totals[frame] + jnp.dot(taps, window, preferred_element_type=jnp.float32)
    return totals


def first_layer(position, own_tiles, partner_tiles, lift_all, lift_own, conv_weight):
    chips = position.shape[0]
    latent = own_tiles.shape[0] // chips
    width = own_tiles.shape[1]
    channels, own_channels = (lift_all.shape[0], lift_own.shape[0])
    taps = conv_weight.shape[1]

    def kernel(
        position_ref, own_ref, partner_ref, all_ref, mine_ref, weight_ref, active_ref, feature_ref,
        weights, windows, sem,
    ):
        third = taps // 3
        copies = [
            pltpu.make_async_copy(
                weight_ref.at[0, pl.ds(part * third, third)], weights.at[pl.ds(part * third, third)], sem.at[part]
            )
            for part in range(3)
        ]
        for copy in copies:
            copy.start()
        row, core = (lax.axis_index("seq"), lax.axis_index("rep"))

        def tile_of(source, target):
            picked = jnp.zeros((latent, width), jnp.float32)
            for piece in range(chips):
                tile = source[pl.ds(piece * latent, latent), :].astype(jnp.float32)
                named = position_ref[neighbour(chips, row, -piece)]
                picked = jnp.where(named == target, tile, picked)
            return picked

        weight_all = all_ref[:, :latent].astype(jnp.bfloat16)
        bias_all = all_ref[:, latent : latent + 1]
        grid = [[None] * 5, [None] * 5]
        for offset in range(5):
            target = row + offset - 2
            inside = jnp.logical_and(target >= 0, target < chips)
            mine, other = (tile_of(own_ref, target), tile_of(partner_ref, target))
            grid[0][offset] = jnp.where(core == 0, mine, other).astype(jnp.bfloat16)
            grid[1][offset] = jnp.where(core == 0, other, mine).astype(jnp.bfloat16)
            for frame in range(2):
                lifted = (
                    jnp.dot(weight_all, grid[frame][offset], preferred_element_type=jnp.float32) + bias_all
                )
                active = jnp.where(inside, silu(lifted), 0.0)
                store_shifted(windows, frame * 5 + offset, active, 0, channels)
        weight_own = mine_ref[:, :latent].astype(jnp.bfloat16)
        bias_own = mine_ref[:, latent : latent + 1]
        totals = [jnp.zeros((own_channels, 3 * width), jnp.float32) for _ in range(2)]
        for frame_tap in range(3):
            copies[frame_tap].wait()
            totals = frame_taps(weights, windows, frame_tap, width, 5, 3, totals)
        for frame in range(2):
            near = jnp.concatenate(grid[frame][1:4], axis=1)
            feature = (
                jnp.dot(weight_own, near, preferred_element_type=jnp.float32) + bias_own
            ) + totals[frame]
            feature_ref[:, pl.ds(frame * width, width)] = feature[:, width : 2 * width]
            for offset in range(3):
                target = row + offset - 1
                inside = jnp.logical_and(target >= 0, target < chips)
                block = silu(feature[:, offset * width : (offset + 1) * width])
                active_ref[:, pl.ds((frame * 3 + offset) * width, width)] = jnp.where(
                    inside, block, 0.0
                ).astype(jnp.bfloat16)

    return pl.pallas_call(
        kernel,
        out_shape=[
            jax.ShapeDtypeStruct((own_channels, 6 * width), jnp.bfloat16),
            jax.ShapeDtypeStruct((own_channels, 2 * width), jnp.float32),
        ],
        in_specs=[pl.BlockSpec(memory_space=pltpu.SMEM)] + whole_vmem(4) + in_hbm(1),
        out_specs=whole_vmem(2),
        scratch_shapes=[
            pltpu.VMEM((taps, own_channels, channels), jnp.bfloat16),
            pltpu.VMEM((3 * channels, 10 * width), jnp.bfloat16),
            pltpu.SemaphoreType.DMA((3,)),
        ],
        compiler_params=limit(24),
        name="first_layer",
    )(position, own_tiles, partner_tiles, lift_all, lift_own, kept(conv_weight))


def second_layer(blocks, feature, conv_weight):
    own_channels = feature.shape[0]
    channels = own_channels * len(blocks)
    width = blocks[0].shape[1] // 6
    taps = conv_weight.shape[1]

    def kernel(*refs):
        inputs = refs[: len(blocks)]
        feature_ref, weight_ref, decoded_ref, weights, windows, sem = refs[len(blocks) :]
        third = taps // 3
        copies = [
            pltpu.make_async_copy(
                weight_ref.at[1, pl.ds(part * third, third)], weights.at[pl.ds(part * third, third)], sem.at[part]
            )
            for part in range(3)
        ]
        for copy in copies:
            copy.start()
        at = 2 * lax.axis_index("head") + lax.axis_index("rep")
        for index, source in enumerate(inputs):
            first = pl.multiple_of(jnp.bitwise_xor(at, index) * own_channels, own_channels)
            for block in range(6):
                store_shifted(
                    windows, block, source[:, pl.ds(block * width, width)].astype(jnp.float32), first, channels
                )
        totals = [jnp.zeros((own_channels, width), jnp.float32) for _ in range(2)]
        for frame_tap in range(3):
            copies[frame_tap].wait()
            totals = frame_taps(weights, windows, frame_tap, width, 3, 1, totals)
        for frame in range(2):
            decoded_ref[:, frame, :] = feature_ref[:, pl.ds(frame * width, width)] + totals[frame]

    return pl.pallas_call(
        kernel,
        out_shape=jax.ShapeDtypeStruct((own_channels, 2, width), jnp.float32),
        in_specs=whole_vmem(len(blocks) + 1) + in_hbm(1),
        out_specs=pl.BlockSpec(memory_space=pltpu.VMEM),
        scratch_shapes=[
            pltpu.VMEM((taps, own_channels, channels), jnp.bfloat16),
            pltpu.VMEM((3 * channels, 6 * width), jnp.bfloat16),
            pltpu.SemaphoreType.DMA((3,)),
        ],
        compiler_params=limit(16),
        name="second_layer",
    )(*blocks, feature, kept(conv_weight))


def exchanged_shards(
    queries,
    key_tokens,
    value_tokens,
    stream,
    norm_gain,
    latent_weight,
    tile_pool,
    tile_position,
    lift_weight,
    lift_bias,
    conv_weight,
):
    chips = lax.axis_size("seq")
    rows = queries.shape[0]
    per_chip = queries.shape[1] // HEAD_DIM // chips
    count = per_chip // 2
    latent_channels = tile_pool.shape[1]
    ring = ring_of(chips)
    onward = [[(ring[at], ring[(at + shift) % chips]) for at in range(chips)] for shift in range(chips)]
    back = [[(target, source) for source, target in pairs] for pairs in onward]
    swap = [(0, 1), (1, 0)]
    sources = (queries, key_tokens, value_tokens)

    def send(messages, permutations):
        arrived = [messages[0]]
        for shift in range(1, chips):
            arrived.append(lax.ppermute(messages[shift], "seq", permutations[shift]))
        return arrived

    early = pack(sources, tile_pool, chips, per_chip, 0, count)
    late = pack(sources, None, chips, per_chip, count, count)
    early_in, late_in = (send(early, onward), send(late, onward))

    lift_weight, lift_bias, _ = lax.optimization_barrier((lift_weight, lift_bias, late[0]))
    lift_own = jnp.concatenate(
        [
            lift_weight.T.astype(jnp.float32),
            lift_bias[:, None],
            jnp.zeros((lift_bias.shape[0], 128 - latent_channels - 1), jnp.float32),
        ],
        axis=1,
    )
    lift_all = lax.all_gather(lift_own, ("head", "rep"), axis=0, tiled=True)

    early_in, lift_all = lax.optimization_barrier((early_in, lift_all))
    own = join(early_in, count, rows, latent_channels)
    partner = lax.ppermute(own, "rep", swap)
    tiles_at = 2 * count * chips * rows
    active, feature = first_layer(tile_position, own[tiles_at:], partner[tiles_at:], lift_all, lift_own, conv_weight)
    core_active = lax.ppermute(active, "rep", swap)
    chip_active = lax.ppermute(active, "head", swap)
    early_out = attend(early_in, own, partner, count, rows)
    early_home = send(early_out, back)

    late_in, _ = lax.optimization_barrier((late_in, early_out[0]))
    own = join(late_in, count, rows, 0)
    partner = lax.ppermute(own, "rep", swap)
    late_out = attend(late_in, own, partner, count, rows)
    late_home = send(late_out, back)

    chip_active, _ = lax.optimization_barrier((chip_active, late_out[0]))
    far_active = lax.ppermute(chip_active, "rep", swap)
    decoded = second_layer((active, core_active, chip_active, far_active), feature, conv_weight)
    decoded = decoded[:, :, None, :]

    hidden, part = close(
        (early_home, late_home), stream, norm_gain[None, :], latent_weight.T, (count, count), per_chip
    )
    part = part + lax.ppermute(part, "head", swap)
    latent = latent_weight.shape[1]
    latents = part[:latent] * lax.rsqrt(part[latent : latent + 1] / WIDTH + epsilon)
    return (hidden, latents.T, decoded)


def shards(*arrays):
    form = exchanged_shards if fits(arrays[0], arrays[6]) else gathered_shards
    return form(*arrays)


def solution(mesh):
    in_specs = (
        P(("groups", "seq", "rep"), "head"),
        P(("groups", "seq", "rep"), "head"),
        P(("groups", "seq", "rep"), "head"),
        P(("groups", "seq", "rep"), "head"),
        P("head"),
        P("head", None),
        P(("groups", "seq"), None, None, None),
        P("groups"),
        P(None, ("head", "rep")),
        P(("head", "rep")),
        P(None, None, ("head", "rep"), None),
    )
    out_specs = (
        P(("groups", "seq", "rep"), "head"),
        P(("groups", "seq", "rep"), None),
        P(("groups", "head", "rep"), None, "seq", None),
    )
    return jax.shard_map(shards, mesh=mesh, in_specs=in_specs, out_specs=out_specs, check_vma=False)
```
